32 devices in a mesh: row: 4 (over x, core), col: 8 (over z, y).
Axes of the slice: x: 2, y: 2, z: 4, core: 2. Of those that a mesh axis runs over, the one named last changes fastest.
Arguments:
- jump: float32 [3, 256, 1024], P(None, 'row', 'col'), may hold values from -6 to 6
- external: float32 [3, 256, 1024], P(None, 'row', 'col'), may hold values from -12 to 12
- cohesive: float32 [256, 1024], P('row', 'col'), may hold values from 0.5 to 4
- bond_mask: int32 [2, 256, 1024], P(None, 'row', 'col'), may hold values 0 or 1
- load_factor: float32 [1], replicated, may hold values from 0.5 to 1.5
- arc_radius: float32 [1], replicated, may hold values from 0.5 to 1.5
- stiffness: bfloat16 [1536, 1536], replicated, may hold values from -1 to 2
- coupling: float32 [3, 1536], replicated, may hold values from -6 to 6
- old_state: float32 [5120, 1536], P(('row', 'col')), may hold values from -3 to 3
- old_history: float32 [5120, 1536], P(('row', 'col')), may hold values from 0 to 1.5
- newton_steps: int32 [5120], P(('row', 'col')), may hold values from 0 to 9, as said below
- point_ids: int32 [5120], P(('row', 'col')), may hold values from 0 to 8191, as said below
Outputs:
- new_jump: float32 [3, 256, 1024], P(None, 'row', 'col')
- new_load: float32 [1], replicated
- new_state: float32 [2560, 1536], P(('row', 'col'))
- new_history: float32 [2560, 1536], P(('row', 'col'))
The draws below stay inside these ranges and needn't reach their ends.
Inputs may be any that keep to these rules, and one draw needn't show every extreme that they name: `newton_steps`: within one block the live slots number between 20 and 160, and some block has all 160 live; in all at most 2240 slots are live; a live slot's count is at least 2. `point_ids`: the slots of one block name distinct points of that block.
All inputs are finite; a program needn't handle non-finite values. No bound on the sum of `bond_mask` on one device may be relied on, other than what follows from the above.
Results may differ from the reference program's by a relative error of at most 0.0028.
Values sent between devices are 32-bit elements; how exact they have to be, the bound alone decides.
A program may use at most 64 MiB of HBM per device.

```python
import math
import jax
import jax.numpy as jnp
from jax import lax

CELLS = 1536
S_CAP = 160
PX = 64
PY = 128
MAX_STEPS = 9
SWEEPS = 3
NEW_CAP = 80
GX = 256
GY = 1024
SLOTS = 5120
NEW_SLOTS = 2560
N_ROW = 4
N_COL = 8


def draw_stiffness(key, part):
    first, second = jax.random.split(jax.random.fold_in(key, 11))
    noise = jax.random.normal(first, (CELLS, CELLS), jnp.float32) * (0.3 / math.sqrt(CELLS))
    symmetric = (noise + noise.T) / math.sqrt(2.0)
    leading = jax.random.uniform(second, (CELLS,), jnp.float32, 1.0, 2.0)
    identity = jnp.eye(CELLS, dtype=jnp.float32)
    return (symmetric * (1.0 - identity) + identity * leading[None, :]).astype(jnp.bfloat16)


def draw_external(key, part):
    shape = (3, GX, GY)
    position = jnp.arange(GX, dtype=jnp.float32)[None, :, None] / GX
    inner = jax.random.fold_in(key, 17)
    rough = jnp.clip(jax.random.normal(inner, shape, jnp.float32), -4.0, 4.0)
    return rough * (1.0 + 2.0 * position)


def draw_newton_steps(key, part):
    blocks = SLOTS // S_CAP
    order_key, size_key, place_key, step_key = jax.random.split(jax.random.fold_in(key, 29), 4)
    order = jax.random.permutation(order_key, blocks)
    crowded = order < blocks // 4
    sparse = jax.random.randint(size_key, (blocks,), S_CAP // 8, S_CAP // 4 + 1)
    held = jnp.where(crowded, S_CAP, sparse)

    def arrange(inner):
        return jax.random.permutation(inner, S_CAP)
    places = jax.vmap(arrange)(jax.random.split(place_key, blocks))
    occupied = places < held[:, None]
    counts = jax.random.randint(step_key, (blocks, S_CAP), 2, MAX_STEPS + 1)
    return jnp.where(occupied, counts, 0).reshape(SLOTS).astype(jnp.int32)


def draw_point_ids(key, part):
    blocks = SLOTS // S_CAP

    def choose(inner):
        return jax.random.permutation(inner, PX * PY)[:S_CAP]
    keys = jax.random.split(jax.random.fold_in(key, 31), blocks)
    return jax.vmap(choose)(keys).reshape(SLOTS).astype(jnp.int32)


def set_ends(values, stream_key, least, largest):
    extent = values.shape
    place = [jax.random.randint(jax.random.fold_in(stream_key, axis), (), 0, extent[axis]) for axis in range(len(extent))]
    values = values.at[tuple(place)].set(least)
    longest = extent.index(max(extent))
    place[longest] = (place[longest] + 1) % extent[longest]
    return values.at[tuple(place)].set(largest)


def block_levels(own_key, dims, cuts, least, top_value):
    def one(dim, shards_of):
        steps = jax.random.uniform(jax.random.fold_in(jax.random.fold_in(own_key, 6), dim), (shards_of,), jnp.float32, least / len(cuts), top_value / len(cuts))
        return jnp.repeat(jnp.exp(steps), dims[dim] // shards_of).reshape((-1,) + (1,) * (len(dims) - dim - 1))

    loudness = one(*cuts[0])
    for cut in cuts[1:]:
        loudness = loudness * one(*cut)
    return loudness


def scatter_about(stream_key, shape, spread, limit, pieces=(), kind=jnp.bfloat16):
    values = jax.random.normal(stream_key, shape, jnp.float32) * spread
    if len(pieces) > 0:
        values = block_levels(stream_key, shape, pieces, -0.22, 0.18) * values
    return jnp.clip(values, min=-limit, max=limit).astype(kind)


def setup_inputs(seed: int = 0) -> dict:
    streams_of = jax.random.split(jax.random.key(seed), 13)
    return {
        "jump": scatter_about(streams_of[0], (3, GX, GY), 1.0, 6.0, ((1, 4), (2, 8)), jnp.float32),
        "external": draw_external(jax.random.fold_in(streams_of[12], 71), 0),
        "cohesive": jnp.clip(jnp.exp(math.log(4.0) - 2.0794415 * jax.random.uniform(streams_of[2], (GX, GY), jnp.float32) ** block_levels(streams_of[2], (GX, GY), ((0, 4), (1, 8)), -0.2, 0.2)), 0.5, 4.0),
        "bond_mask": set_ends((jax.random.randint(streams_of[3], (2, GX, GY), 0, 4) < 3).astype(jnp.int32), jax.random.fold_in(streams_of[3], 1), 0, 1),
        "load_factor": jnp.clip(jax.random.uniform(streams_of[4], (1,), jnp.float32, 0.5, 1.5), 0.5, 1.5),
        "arc_radius": jnp.clip(jax.random.uniform(streams_of[5], (1,), jnp.float32, 0.5, 1.5), 0.5, 1.5),
        "stiffness": draw_stiffness(jax.random.fold_in(streams_of[12], 71), 0),
        "coupling": scatter_about(streams_of[7], (3, CELLS), 1.0, 6.0, (), jnp.float32),
        "old_state": scatter_about(streams_of[8], (SLOTS, CELLS), 0.5, 3.0, ((0, 32),), jnp.float32),
        "old_history": jnp.clip(1.5 * jax.random.uniform(streams_of[9], (SLOTS, CELLS), jnp.float32) ** block_levels(streams_of[9], (SLOTS, CELLS), ((0, 32),), -0.2, 0.2), 0.0, 1.5),
        "newton_steps": draw_newton_steps(jax.random.fold_in(streams_of[12], 71), 0),
        "point_ids": draw_point_ids(jax.random.fold_in(streams_of[12], 71), 0),
    }


softening = 1.0

def micro_solve(state, history, drive, steps, stiffness, coupling):
    diagonal = jnp.diagonal(stiffness).astype(jnp.float32)
    load = jnp.dot(drive, coupling, precision=lax.Precision.HIGHEST)
    damage = jnp.exp(-history)

    def advance(count, current):
        bent = jnp.tanh(current)
        force = jnp.dot(current.astype(jnp.bfloat16), stiffness, preferred_element_type=jnp.float32)
        misfit = force + softening * damage * bent - load
        slope = diagonal + softening * damage * (1.0 - bent * bent)
        return jnp.where((count < steps)[:, None], current - misfit / slope, current)
    state = lax.fori_loop(0, MAX_STEPS, advance, state)
    bent = jnp.tanh(state)
    cells = state.shape[1]
    traction = jnp.dot(softening * damage * bent, coupling.T, precision=lax.Precision.HIGHEST) / cells
    weight = softening * damage * (1.0 - bent * bent)
    products = jnp.stack([coupling[0] * coupling[0], coupling[1] * coupling[1], coupling[2] * coupling[2], coupling[0] * coupling[1], coupling[0] * coupling[2], coupling[1] * coupling[2]])
    tangent = jnp.dot(weight, products.T, precision=lax.Precision.HIGHEST) / cells
    history = jnp.maximum(history, jnp.abs(state))
    return (state, history, traction, tangent)

def block_solve(scale, tangent, source):
    d00 = scale + tangent[0]
    d11 = scale + tangent[1]
    d22 = scale + tangent[2]
    d01, d02, d12 = (tangent[3], tangent[4], tangent[5])
    c00 = d11 * d22 - d12 * d12
    c11 = d00 * d22 - d02 * d02
    c22 = d00 * d11 - d01 * d01
    c01 = d02 * d12 - d01 * d22
    c02 = d01 * d12 - d02 * d11
    c12 = d01 * d02 - d00 * d12
    determinant = d00 * c00 + d01 * c01 + d02 * c02
    first = (c00 * source[0] + c01 * source[1] + c02 * source[2]) / determinant
    second = (c01 * source[0] + c11 * source[1] + c12 * source[2]) / determinant
    third = (c02 * source[0] + c12 * source[1] + c22 * source[2]) / determinant
    return jnp.stack([first, second, third])

def neighbours(field, bond_x, low_x, bond_y, low_y):
    padded = jnp.pad(field, ((0, 0), (1, 1), (1, 1)))
    return bond_x * padded[:, 2:, 1:-1] + low_x * padded[:, :-2, 1:-1] + bond_y * padded[:, 1:-1, 2:] + low_y * padded[:, 1:-1, :-2]

def reference(jump, external, cohesive, bond_mask, load_factor, arc_radius, stiffness, coupling, old_state, old_history, newton_steps, point_ids):
    devices = N_ROW * N_COL
    slot_block = jnp.arange(SLOTS, dtype=jnp.int32) // S_CAP
    grid_x = slot_block // N_COL * PX + point_ids // PY
    grid_y = slot_block % N_COL * PY + point_ids % PY
    drive = jump[:, grid_x, grid_y].T
    live = newton_steps > 0
    live_float = live.astype(jnp.float32)

    def per_block(block):
        return micro_solve(block[0], block[1], block[2], block[3], stiffness, coupling)
    blocks = (old_state.reshape(devices, S_CAP, CELLS), old_history.reshape(devices, S_CAP, CELLS), drive.reshape(devices, S_CAP, 3), newton_steps.reshape(devices, S_CAP))
    state, history, traction, tangent = lax.map(per_block, blocks)
    state = state.reshape(SLOTS, CELLS)
    history = history.reshape(SLOTS, CELLS)
    traction = traction.reshape(SLOTS, 3)
    tangent = tangent.reshape(SLOTS, 6)
    soft = jnp.zeros((GX, GY), jnp.float32).at[grid_x, grid_y].add(live_float)
    rve_traction = jnp.zeros((3, GX, GY), jnp.float32).at[:, grid_x, grid_y].add((traction * live_float[:, None]).T)
    rve_tangent = jnp.zeros((6, GX, GY), jnp.float32).at[:, grid_x, grid_y].add((tangent * live_float[:, None]).T)
    bond_x = 0.25 + 0.75 * bond_mask[0].astype(jnp.float32)
    bond_y = 0.25 + 0.75 * bond_mask[1].astype(jnp.float32)
    low_x = jnp.pad(bond_x, ((1, 0), (0, 0)))[:-1]
    low_y = jnp.pad(bond_y, ((0, 0), (1, 0)))[:, :-1]
    scale = bond_x + low_x + bond_y + low_y + (1.0 - soft) * cohesive
    residual = scale * jump - neighbours(jump, bond_x, low_x, bond_y, low_y) + rve_traction - load_factor[0] * external
    source = jnp.concatenate([-residual, external])

    def solve_both(values):
        return jnp.concatenate([block_solve(scale, rve_tangent, values[:3]), block_solve(scale, rve_tangent, values[3:])])
    iterate = solve_both(source)
    for sweep in range(SWEEPS):
        iterate = solve_both(source + neighbours(iterate, bond_x, low_x, bond_y, low_y))
    correction, direction = (iterate[:3], iterate[3:])
    cross = jnp.sum(correction * direction)
    square = jnp.sum(direction * direction)
    entries = 3.0 * GX * GY
    shifted = square + 0.25 * entries
    increment = (arc_radius[0] * jnp.sqrt(entries) * jnp.sqrt(shifted) - cross) / shifted
    new_jump = jump + correction + increment * direction
    new_load = load_factor + increment
    live_int = live.astype(jnp.int32)
    rank = jnp.cumsum(live_int, dtype=jnp.int32) - live_int
    home_block = rank // 2 % devices
    home_slot = 2 * (rank // (2 * devices)) + rank % 2
    target = jnp.where(live, home_block * NEW_CAP + home_slot, NEW_SLOTS).astype(jnp.int32)
    new_state = jnp.zeros((NEW_SLOTS, CELLS), jnp.float32).at[target].set(state, mode='drop')
    new_history = jnp.zeros((NEW_SLOTS, CELLS), jnp.float32).at[target].set(history, mode='drop')
    return (new_jump, new_load, new_state, new_history)
```

```python
import functools

import jax
import jax.numpy as jnp
from jax import lax
from jax.experimental import pallas as pl
from jax.experimental.pallas import tpu as pltpu
from jax.sharding import PartitionSpec as P

MAX_STEPS = 9
SWEEPS = 3
TILE = 256
LANES = 128
MESH = pl.DeviceIdType.MESH
F32 = jnp.float32
BF16 = jnp.bfloat16
HIGHEST = lax.Precision.HIGHEST


def iota(shape, dim):
    return lax.broadcasted_iota(jnp.int32, shape, dim)


def picked(onehot, values):
    high = values.astype(BF16)
    rest = values - high.astype(F32)
    middle = rest.astype(BF16)
    low = (rest - middle.astype(F32)).astype(BF16)
    dot = functools.partial(jnp.dot, preferred_element_type=F32)
    return dot(onehot, high) + dot(onehot, middle) + dot(onehot, low)


def body(
    nrow,
    ncol,
    pair,
    jump_ref,
    external_ref,
    cohesive_ref,
    bond_ref,
    load_ref,
    radius_ref,
    coupling_ref,
    steps_ref,
    points_ref,
    stiffness_hbm,
    state_hbm,
    history_hbm,
    new_jump_ref,
    new_load_ref,
    new_state_ref,
    new_history_ref,
    stiff,
    state,
    history,
    damage,
    load,
    rounded,
    diagonal,
    count_out,
    count_in,
    sum_out,
    sum_in,
    x_out,
    x_in,
    y_out,
    y_in,
    out_history,
    in_history,
    out_state,
    in_state,
    local_sems,
    halo_send,
    halo_recv,
    all_send,
    all_recv,
):
    devices = nrow * ncol
    row, col = lax.axis_index("row"), lax.axis_index("col")
    here = row * ncol + col
    slots, cells = state.shape
    X, Y = cohesive_ref.shape
    new_cap = new_state_ref.shape[0]
    padded = out_history.shape[1]
    width = devices * padded
    bits = devices.bit_length() - 1

    fetch = [
        pltpu.make_async_copy(history_hbm, history, local_sems.at[0]),
        pltpu.make_async_copy(stiffness_hbm, stiff, local_sems.at[1]),
        pltpu.make_async_copy(state_hbm, state, local_sems.at[2]),
    ]
    for copy in fetch:
        copy.start()

    def peer(k):
        p = lax.rem(here + k, devices)
        return {"row": lax.div(p, ncol), "col": lax.rem(p, ncol)}, p

    x_in[...] = jnp.zeros_like(x_in)
    y_in[...] = jnp.zeros_like(y_in)
    if pair < padded:
        blank = jnp.zeros((devices, padded - pair, cells), F32)
        in_history[:, pair:, :] = blank
        in_state[:, pair:, :] = blank

    steps_row = steps_ref[...]
    live_row = (steps_row > 0).astype(F32)
    count_out[...] = jnp.broadcast_to(jnp.sum(live_row, axis=1, keepdims=True), count_out.shape)

    lane = iota((X, Y), 1)
    line = iota((X, Y), 0)

    def stage(phase, fields):
        right = jnp.zeros((X, Y), F32)
        left = jnp.zeros((X, Y), F32)
        for c, (x_field, y_field) in enumerate(fields):
            x_out[phase, 0, c : c + 1, :] = x_field[X - 1 : X, :]
            x_out[phase, 1, c : c + 1, :] = x_field[0:1, :]
            right = jnp.where(lane == c, pltpu.roll(y_field, (c + 1) % Y, 1), right)
            left = jnp.where(lane == c, pltpu.roll(y_field, c, 1), left)
        y_out[phase, 0] = right
        y_out[phase, 1] = left

    def halo_copies(phase):
        plan = (
            (x_out, x_in, 0, row < nrow - 1, row > 0, {"row": row + 1, "col": col}),
            (x_out, x_in, 1, row > 0, row < nrow - 1, {"row": row - 1, "col": col}),
            (y_out, y_in, 0, col < ncol - 1, col > 0, {"row": row, "col": col + 1}),
            (y_out, y_in, 1, col > 0, col < ncol - 1, {"row": row, "col": col - 1}),
        )
        copies = []
        for index, (source, target, way, sends, gets, device) in enumerate(plan):
            copy = pltpu.make_async_remote_copy(
                src_ref=source.at[phase, way],
                dst_ref=target.at[phase, way],
                send_sem=halo_send.at[phase, index],
                recv_sem=halo_recv.at[phase, index],
                device_id=device,
                device_id_type=MESH,
            )
            copies.append((copy, sends, gets))
        return copies

    def halo_start(phase):
        for copy, sends, _ in halo_copies(phase):
            pl.when(sends)(copy.start)

    def halo_wait(phase):
        for copy, sends, gets in halo_copies(phase):
            pl.when(gets)(copy.wait_recv)

    def halo_wait_sends(phase):
        for copy, sends, gets in halo_copies(phase):
            pl.when(sends)(copy.wait_send)

    def spread(source_of, target, kind, first, last):
        def one(k, carry):
            device, p = peer(k)
            pltpu.make_async_remote_copy(
                src_ref=source_of(p),
                dst_ref=target,
                send_sem=all_send.at[kind],
                recv_sem=all_recv.at[kind],
                device_id=device,
                device_id_type=MESH,
            ).start()
            return carry

        lax.fori_loop(first, last, one, 0)

    def spread_wait(buffer, sem):
        pltpu.make_async_copy(buffer, buffer, sem).wait()

    bond_x = 0.25 + 0.75 * bond_ref[0].astype(F32)
    bond_y = 0.25 + 0.75 * bond_ref[1].astype(F32)
    jump = [jump_ref[c] for c in range(3)]
    stage(0, [(jump[c], jump[c]) for c in range(3)] + [(bond_x, bond_y)])

    barrier = pltpu.get_barrier_semaphore()

    def greet(k, carry):
        device, _ = peer(k)
        pl.semaphore_signal(barrier, inc=1, device_id=device, device_id_type=MESH)
        return carry

    lax.fori_loop(1, devices, greet, 0)
    pl.semaphore_wait(barrier, devices - 1)

    count_in[pl.ds(here, 1)] = count_out[...][None]
    spread(lambda p: count_out, count_in.at[here], 0, 1, devices)
    halo_start(0)

    slot_line = iota((slots, slots), 0)
    slot_lane = iota((slots, slots), 1)

    def to_column(values):
        return jnp.sum(jnp.where(slot_line == slot_lane, values, 0.0), axis=1, keepdims=True)

    points_row = points_ref[...]
    px_row = lax.shift_right_logical(points_row, (Y.bit_length() - 1))
    py_row = points_row & (Y - 1)
    px_col = to_column(px_row.astype(F32)).astype(jnp.int32)
    py_col = to_column(py_row.astype(F32)).astype(jnp.int32)
    steps_col = to_column(steps_row.astype(F32)).astype(jnp.int32)
    live_col = (steps_col > 0).astype(F32)
    at_x = (iota((slots, X), 1) == px_col).astype(F32)
    at_y = (iota((slots, Y), 1) == py_col).astype(F32)
    at_x_turned = (iota((X, slots), 0) == px_row).astype(F32)
    drive = []
    for c in range(3):
        lines = jnp.dot(at_x, jump[c], precision=HIGHEST, preferred_element_type=F32)
        drive.append(jnp.sum(lines * at_y, axis=1, keepdims=True))
    for start in range(0, cells, TILE):
        part = slice(start, start + TILE)
        total = drive[0] * coupling_ref[0:1, part]
        total = total + drive[1] * coupling_ref[1:2, part]
        load[:, part] = total + drive[2] * coupling_ref[2:3, part]
    rank_row = jnp.sum(jnp.where(slot_line < slot_lane, live_col, 0.0), axis=0, keepdims=True)

    fetch[0].wait()
    for start in range(0, cells, TILE):
        part = slice(start, start + TILE)
        damage[:, part] = jnp.exp(-history[:, part])

    spread_wait(count_in.at[pl.ds(0, devices - 1)], all_recv.at[0])
    counts = jnp.max(count_in[...], axis=1)
    device_line = iota((devices, LANES), 0)
    device_lane = iota((devices, LANES), 1)
    starts = jnp.sum(jnp.where(device_line < device_lane, counts, 0.0), axis=0, keepdims=True)
    ends = jnp.sum(jnp.where(device_line <= device_lane, counts, 0.0), axis=0, keepdims=True)
    my_start = jnp.sum(jnp.where(device_line < here, counts, 0.0), axis=0, keepdims=True)[:, :1]
    my_start = my_start.astype(jnp.int32)

    def place(rank, first):
        pairs = lax.shift_right_logical(rank, 1) - lax.shift_right_logical(first, 1)
        return 2 * lax.shift_right_logical(pairs, bits) + (rank & 1)

    ranks = rank_row.astype(jnp.int32) + my_start
    home = lax.shift_right_logical(ranks, 1) & (devices - 1)
    leaves = jnp.where(steps_row > 0, home * padded + place(ranks, my_start), -1)
    leaving = (iota((width, slots), 0) == leaves).astype(F32).astype(BF16)

    wanted_slot = iota((new_cap, LANES), 0)
    wanted = 2 * (here + devices * lax.shift_right_logical(wanted_slot, 1)) + (wanted_slot & 1)
    wanted_lane = iota((new_cap, LANES), 1)
    wanted_float = wanted.astype(F32)
    hit = (starts <= wanted_float) & (wanted_float < ends) & (wanted_lane < devices)
    valid = jnp.sum(jnp.where(hit, 1.0, 0.0), axis=1, keepdims=True)
    from_start = jnp.sum(jnp.where(hit, starts, 0.0), axis=1, keepdims=True).astype(jnp.int32)
    source = jnp.sum(jnp.where(hit, wanted_lane.astype(F32), 0.0), axis=1, keepdims=True)
    arrives = source.astype(jnp.int32) * padded + place(wanted[:, :1], from_start)
    arrives = jnp.where(valid > 0.0, arrives, -1)
    coming = (iota((new_cap, width), 1) == arrives).astype(F32).astype(BF16)

    def gather_out(values, out, inside):
        for start in range(0, cells, TILE):
            part = slice(start, start + TILE)
            rows = picked(leaving, values[:, part])
            out[:, :, part] = rows.reshape(devices, padded, TILE)
        inside[pl.ds(here, 1)] = out[pl.ds(here, 1)]

    gather_out(history, out_history, in_history)
    row_part = pl.ds(0, pair)
    spread(
        lambda p: out_history.at[p, row_part], in_history.at[here, row_part], 1, 1, devices
    )

    fetch[1].wait()
    fetch[2].wait()
    tile_eye = iota((TILE, TILE), 0) == iota((TILE, TILE), 1)
    for start in range(0, cells, TILE):
        part = slice(start, start + TILE)
        block = stiff[part, part].astype(F32)
        diagonal[:, part] = jnp.sum(jnp.where(tile_eye, block, 0.0), axis=0, keepdims=True)
        rounded[0, :, part] = state[:, part].astype(BF16)

    def advance(count, carry):
        now = lax.rem(count, 2)
        moves = count < steps_col
        for start in range(0, cells, TILE):
            part = slice(start, start + TILE)
            force = jnp.dot(rounded[now], stiff[:, part], preferred_element_type=F32)
            current = state[:, part]
            bent = jnp.tanh(current)
            worn = damage[:, part]
            misfit = force + worn * bent - load[:, part]
            slope = diagonal[:, part] + worn * (1.0 - bent * bent)
            current = jnp.where(moves, current - misfit / slope, current)
            state[:, part] = current
            rounded[1 - now, :, part] = current.astype(BF16)
        return carry

    lax.fori_loop(0, MAX_STEPS, advance, 0)

    first_sum = jnp.zeros((slots, 8), F32)
    second_sum = jnp.zeros((slots, 8), F32)
    turned = (((1,), (1,)), ((), ()))
    for start in range(0, cells, TILE):
        part = slice(start, start + TILE)
        bent = jnp.tanh(state[:, part])
        worn = damage[:, part]
        a0, a1, a2 = [coupling_ref[a : a + 1, part] for a in range(3)]
        none = jnp.zeros((2, TILE), F32)
        firsts = jnp.concatenate([a0, a1, a2, none, none, none[:1]], axis=0)
        seconds = jnp.concatenate(
            [a0 * a0, a1 * a1, a2 * a2, a0 * a1, a0 * a2, a1 * a2, none], axis=0
        )
        first_sum = first_sum + lax.dot_general(
            worn * bent, firsts, turned, precision=HIGHEST, preferred_element_type=F32
        )
        second_sum = second_sum + lax.dot_general(
            worn * (1.0 - bent * bent),
            seconds,
            turned,
            precision=HIGHEST,
            preferred_element_type=F32,
        )
    first_sum = first_sum * (live_col / cells)
    second_sum = second_sum * (live_col / cells)

    def put(values):
        return jnp.dot(at_x_turned, at_y * values, precision=HIGHEST, preferred_element_type=F32)

    soft = put(live_col)
    rve_traction = [put(first_sum[:, c : c + 1]) for c in range(3)]
    tangent = [put(second_sum[:, c : c + 1]) for c in range(6)]

    halo_wait(0)

    def before_x(phase, field, c):
        return jnp.where(line == 0, x_in[phase, 0, c : c + 1, :], pltpu.roll(field, 1, 0))

    def after_x(phase, field, c):
        return jnp.where(line == X - 1, x_in[phase, 1, c : c + 1, :], pltpu.roll(field, X - 1, 0))

    def before_y(phase, field, c):
        edge = pltpu.roll(y_in[phase, 0], (Y - c) % Y, 1)
        return jnp.where(lane == 0, edge, pltpu.roll(field, 1, 1))

    def after_y(phase, field, c):
        edge = pltpu.roll(y_in[phase, 1], Y - 1 - c, 1)
        return jnp.where(lane == Y - 1, edge, pltpu.roll(field, Y - 1, 1))

    low_x = before_x(0, bond_x, 3)
    low_y = before_y(0, bond_y, 3)

    def neighbours(phase, field, c):
        return (
            bond_x * after_x(phase, field, c)
            + low_x * before_x(phase, field, c)
            + bond_y * after_y(phase, field, c)
            + low_y * before_y(phase, field, c)
        )

    scale = bond_x + low_x + bond_y + low_y + (1.0 - soft) * cohesive_ref[...]
    terms = []
    for c in range(3):
        residual = (
            scale * jump[c]
            - neighbours(0, jump[c], c)
            + rve_traction[c]
            - load_ref[0] * external_ref[c]
        )
        terms.append(-residual)
    for c in range(3):
        terms.append(external_ref[c])
    d00, d11, d22 = [scale + tangent[c] for c in range(3)]
    d01, d02, d12 = tangent[3:]
    c00 = d11 * d22 - d12 * d12
    c11 = d00 * d22 - d02 * d02
    c22 = d00 * d11 - d01 * d01
    c01 = d02 * d12 - d01 * d22
    c02 = d01 * d12 - d02 * d11
    c12 = d01 * d02 - d00 * d12
    inverse = 1.0 / (d00 * c00 + d01 * c01 + d02 * c02)
    c00, c11, c22, c01, c02, c12 = [c * inverse for c in (c00, c11, c22, c01, c02, c12)]

    def solve_both(w):
        result = []
        for h in (0, 3):
            result.append(c00 * w[h] + c01 * w[h + 1] + c02 * w[h + 2])
            result.append(c01 * w[h] + c11 * w[h + 1] + c12 * w[h + 2])
            result.append(c02 * w[h] + c12 * w[h + 1] + c22 * w[h + 2])
        return result

    iterate = solve_both(terms)
    bounds = [1 + (devices - 1) * s // SWEEPS for s in range(SWEEPS + 1)]
    for sweep in range(SWEEPS):
        phase = sweep + 1
        stage(phase, [(v, v) for v in iterate])
        halo_start(phase)
        if sweep == 0:
            gather_out(state, out_state, in_state)
        spread(
            lambda p: out_state.at[p, row_part],
            in_state.at[here, row_part],
            2,
            bounds[sweep],
            bounds[sweep + 1],
        )
        halo_wait(phase)
        iterate = solve_both([terms[c] + neighbours(phase, iterate[c], c) for c in range(6)])
    correction, direction = iterate[:3], iterate[3:]

    def total_of(fields):
        return jnp.sum(fields[0] + fields[1] + fields[2], axis=0, keepdims=True)

    cross_row = total_of([correction[c] * direction[c] for c in range(3)])
    square_row = total_of([direction[c] * direction[c] for c in range(3)])
    sum_out[...] = jnp.where(iota((8, Y), 0) == 0, cross_row, square_row)
    sum_in[pl.ds(here, 1)] = sum_out[...][None]
    spread(lambda p: sum_out, sum_in.at[here], 3, 1, devices)
    spread_wait(sum_in.at[pl.ds(0, devices - 1)], all_recv.at[3])
    sums = jnp.sum(sum_in[...], axis=0)
    cross = jnp.sum(sums[0:1, :], axis=1, keepdims=True)
    square = jnp.sum(sums[1:2, :], axis=1, keepdims=True)
    entries = 3.0 * X * Y * devices
    shifted = square + 0.25 * entries
    root = jnp.sqrt(shifted) * (entries**0.5)
    increment = (radius_ref[0] * root - cross) / shifted
    for c in range(3):
        new_jump_ref[c] = jump[c] + correction[c] + increment * direction[c]
    new_load_ref[...] = load_ref[0] + increment

    peers = pl.ds(0, devices - 1)
    spread_wait(in_history.at[peers, row_part], all_recv.at[1])
    spread_wait(in_state.at[peers, row_part], all_recv.at[2])
    for start in range(0, cells, TILE):
        part = slice(start, start + TILE)
        moved = picked(coming, in_state[:, :, part].reshape(width, TILE))
        kept = picked(coming, in_history[:, :, part].reshape(width, TILE))
        new_state_ref[:, part] = moved
        new_history_ref[:, part] = jnp.maximum(kept, jnp.abs(moved))

    for phase in range(SWEEPS + 1):
        halo_wait_sends(phase)
    spread_wait(count_in.at[peers], all_send.at[0])
    spread_wait(out_history.at[peers, row_part], all_send.at[1])
    spread_wait(out_state.at[peers, row_part], all_send.at[2])
    spread_wait(sum_in.at[peers], all_send.at[3])


def on_device(
    jump,
    external,
    cohesive,
    bond_mask,
    load_factor,
    arc_radius,
    stiffness,
    coupling,
    old_state,
    old_history,
    newton_steps,
    point_ids,
):
    nrow, ncol = lax.axis_size("row"), lax.axis_size("col")
    devices = nrow * ncol
    slots, cells = old_state.shape
    X, Y = cohesive.shape
    new_cap = slots // 2
    pair = 2 * ((slots + 2 * devices + 1) // (2 * devices))
    padded = 8 * ((pair + 7) // 8)
    phases = SWEEPS + 1
    vmem = pl.BlockSpec(memory_space=pltpu.VMEM)
    smem = pl.BlockSpec(memory_space=pltpu.SMEM)
    hbm = pl.BlockSpec(memory_space=pl.ANY)
    new_jump, new_load, new_state, new_history = pl.pallas_call(
        functools.partial(body, nrow, ncol, pair),
        out_shape=(
            jax.ShapeDtypeStruct(jump.shape, F32),
            jax.ShapeDtypeStruct((1, 1), F32),
            jax.ShapeDtypeStruct((new_cap, cells), F32),
            jax.ShapeDtypeStruct((new_cap, cells), F32),
        ),
        in_specs=[vmem] * 4 + [smem] * 2 + [vmem] * 3 + [hbm] * 3,
        out_specs=(vmem,) * 4,
        scratch_shapes=[
            pltpu.VMEM((cells, cells), BF16),
            pltpu.VMEM((slots, cells), F32),
            pltpu.VMEM((slots, cells), F32),
            pltpu.VMEM((slots, cells), F32),
            pltpu.VMEM((slots, cells), F32),
            pltpu.VMEM((2, slots, cells), BF16),
            pltpu.VMEM((1, cells), F32),
            pltpu.VMEM((8, LANES), F32),
            pltpu.VMEM((devices, 8, LANES), F32),
            pltpu.VMEM((8, Y), F32),
            pltpu.VMEM((devices, 8, Y), F32),
            pltpu.VMEM((phases, 2, 8, Y), F32),
            pltpu.VMEM((phases, 2, 8, Y), F32),
            pltpu.VMEM((phases, 2, X, Y), F32),
            pltpu.VMEM((phases, 2, X, Y), F32),
            pltpu.VMEM((devices, padded, cells), F32),
            pltpu.VMEM((devices, padded, cells), F32),
            pltpu.VMEM((devices, padded, cells), F32),
            pltpu.VMEM((devices, padded, cells), F32),
            pltpu.SemaphoreType.DMA((3,)),
            pltpu.SemaphoreType.DMA((phases, 4)),
            pltpu.SemaphoreType.DMA((phases, 4)),
            pltpu.SemaphoreType.DMA((4,)),
            pltpu.SemaphoreType.DMA((4,)),
        ],
        compiler_params=pltpu.CompilerParams(
            collective_id=0, has_side_effects=True, vmem_limit_bytes=60 * 1024 * 1024
        ),
    )(
        jump,
        external,
        cohesive,
        bond_mask,
        load_factor,
        arc_radius,
        coupling,
        newton_steps.reshape(1, slots),
        point_ids.reshape(1, slots),
        stiffness,
        old_state,
        old_history,
    )
    return new_jump, new_load.reshape(1), new_state, new_history


def solution(mesh):
    in_specs = (
        P(None, "row", "col"),
        P(None, "row", "col"),
        P("row", "col"),
        P(None, "row", "col"),
        P(),
        P(),
        P(),
        P(),
        P(("row", "col"), None),
        P(("row", "col"), None),
        P(("row", "col")),
        P(("row", "col")),
    )
    out_specs = (P(None, "row", "col"), P(), P(("row", "col"), None), P(("row", "col"), None))
    return jax.shard_map(
        on_device, mesh=mesh, in_specs=in_specs, out_specs=out_specs, check_vma=False
    )
```
